8 devices in a mesh: data: 1 (over z), model: 2 (over y), time: 4 (over x, core).
Axes of the slice: x: 2, y: 2, z: 1, core: 2. Of those that a mesh axis runs over, the one named last changes fastest.
Arguments:
- x_init: float32 [64, 256, 16], P('data')
- w_up: bfloat16 [16, 384], P(None, 'model')
- w_down: bfloat16 [384, 16], P('model')
- mod_scale: bfloat16 [32, 384], P('time', 'model')
- mod_shift: bfloat16 [32, 384], P('time', 'model')
- step_size: float32 [32], P('time')
Outputs:
- output: float32 [32, 64, 256, 16], P('time', 'data')
All inputs are finite; a program needn't handle non-finite values.
Results may differ from the reference program's by a relative error of at most 0.001.
Values are sent between devices in bfloat16 or wider.
A program may use at most 1 GiB of HBM per device.

```python
import jax
import jax.numpy as jnp
from jax import lax

STEPS = 32
BATCH = 64
TOKENS = 256
CHAN = 16
HIDDEN = 384
SWEEPS = 4


def setup_inputs(seed: int = 0, part: int = 0) -> dict:
    base_key = jax.random.key(seed)
    key_list = jax.random.split(base_key, 6)
    part_key = jax.random.fold_in(key_list[5], part)
    x_init = jax.random.normal(part_key, (BATCH, TOKENS, CHAN), jnp.float32)
    w_up = (jax.random.normal(key_list[0], (CHAN, HIDDEN), jnp.float32) * CHAN ** -0.5).astype(jnp.bfloat16)
    w_down = (jax.random.normal(key_list[1], (HIDDEN, CHAN), jnp.float32) * HIDDEN ** -0.5).astype(jnp.bfloat16)
    mod_scale = (0.5 * jax.random.normal(key_list[2], (STEPS, HIDDEN), jnp.float32)).astype(jnp.bfloat16)
    mod_shift = (0.5 * jax.random.normal(key_list[3], (STEPS, HIDDEN), jnp.float32)).astype(jnp.bfloat16)
    step_size = (3.0 / STEPS) * jax.random.uniform(key_list[4], (STEPS,), jnp.float32, 0.2, 1.8)
    return {'x_init': x_init, 'w_up': w_up, 'w_down': w_down, 'mod_scale': mod_scale, 'mod_shift': mod_shift, 'step_size': step_size}


def drift_at(latent, scale_row, shift_row, step_val, w_up, w_down):
    flat_lat = latent.reshape(BATCH * TOKENS, CHAN).astype(jnp.bfloat16)
    pre_act = jnp.dot(flat_lat, w_up, preferred_element_type=jnp.float32)
    hidden = jax.nn.gelu(pre_act * (1.0 + scale_row.astype(jnp.float32)) + shift_row.astype(jnp.float32), approximate=True)
    proj_out = jnp.dot(hidden.astype(jnp.bfloat16), w_down, preferred_element_type=jnp.float32)
    return step_val * proj_out.reshape(BATCH, TOKENS, CHAN)


def reference(x_init, w_up, w_down, mod_scale, mod_shift, step_size):
    def drift_step(packed):
        return drift_at(packed[0], packed[1], packed[2], packed[3], w_up, w_down)

    def one_sweep(latents, unused):
        drifts = lax.map(drift_step, (latents, mod_scale, mod_shift, step_size))
        prefix = jnp.cumsum(drifts, axis=0) - drifts
        return x_init[None] + prefix, unused

    start_lat = jnp.broadcast_to(x_init[None], (STEPS, BATCH, TOKENS, CHAN))
    final_lat, unused = lax.scan(one_sweep, start_lat, None, length=SWEEPS)
    return final_lat
```

```python
import functools
import math

import jax
import jax.numpy as jnp
from jax import lax
from jax.experimental import pallas as pl
from jax.experimental.pallas import tpu as pltpu
from jax.sharding import PartitionSpec as P

MESH = pl.DeviceIdType.MESH
F32 = jnp.float32
BF16 = jnp.bfloat16

STEPS = 32
STEPS_DEV = 8
HALF = 192
HIDDEN = 384
CHAN = 16
TOKENS = 256
TILES = 8
GROUP = 8
GROUPS = 15
DEPTH = 128

ROOT = math.sqrt(2.0 / math.pi)
C1 = 2.0 * ROOT
C3 = 8.0 * 0.044715 * ROOT


def item(group, k):
    n = group * GROUP + k
    sweep0 = n < 31
    j = jnp.where(sweep0, n, jnp.where(n < 61, n - 30, jnp.where(n < 91, n - 60, n - 89)))
    return sweep0, j


def kernel(x_ref, w1_ref, w2_ref, g_ref, b_ref, h_ref, out_ref,
           gam, bet, w1s, w2s, hs, w1f, gamf, betf, mat, w2t, rhs, pre_a, pre_b, act_a, act_b, lat,
           psend, precv, send_sem, recv_sem):
    m = lax.axis_index("model")
    t = lax.axis_index("time")
    me = m * 4 + t

    offsets = [(dm, dt) for dm in range(2) for dt in range(4) if (dm, dt) != (0, 0)]
    peers = [(lax.rem(m + dm, 2), lax.rem(t + dt, 4)) for dm, dt in offsets]

    barrier = pltpu.get_barrier_semaphore()
    for pm, pt in peers:
        pl.semaphore_signal(barrier, inc=1, device_id={"model": pm, "time": pt}, device_id_type=MESH)
    pl.semaphore_wait(barrier, len(peers))

    copies = []

    def push(src, dst, peer):
        idx = len(copies)
        copy = pltpu.make_async_remote_copy(
            src_ref=src, dst_ref=dst, send_sem=psend.at[idx], recv_sem=precv.at[idx],
            device_id={"model": peer[0], "time": peer[1]}, device_id_type=MESH)
        copy.start()
        copies.append(copy)

    for (dm, dt), peer in zip(offsets, peers):
        push(g_ref, gam.at[m, t], peer)
        push(b_ref, bet.at[m, t], peer)
        if dt == 0:
            push(w1_ref, w1s.at[m], peer)
            push(w2_ref, w2s.at[m], peer)
        if dm == 0:
            push(h_ref, hs.at[t], peer)

    gam[m, t] = g_ref[...]
    bet[m, t] = b_ref[...]
    w1s[m] = w1_ref[...]
    w2s[m] = w2_ref[...]
    hs[t] = h_ref[...]
    w1f[...] = jnp.zeros_like(w1f)
    gamf[...] = jnp.zeros_like(gamf)
    betf[...] = jnp.zeros_like(betf)

    ones_zeros = jnp.concatenate([jnp.ones((16, TOKENS), BF16), jnp.zeros((DEPTH - 64, TOKENS), BF16)], axis=0)

    def init_slot(i, c):
        rhs[i, 48:DEPTH, :] = ones_zeros
        return c

    lax.fori_loop(0, STEPS + TILES, init_slot, 0)

    def init_tile(i, c):
        x0 = x_ref[me * TILES + i]
        lat[i, 0] = x0
        xb = x0.astype(BF16)
        for r in range(3):
            rhs[STEPS + i, 16 * r:16 * r + 16, :] = xb
        return c

    lax.fori_loop(0, TILES, init_tile, 0)

    for copy in copies:
        copy.wait()

    for mm in range(2):
        w1f[mm, :, 0:HALF] = w1s[mm].astype(F32) * 0.5
        w2t[mm] = w2s[mm].astype(F32)
        for tt in range(4):
            gamf[mm, 8 * tt:8 * tt + 8, 0:HALF] = gam[mm, tt].astype(F32)
            betf[mm, 8 * tt:8 * tt + 8, 0:HALF] = bet[mm, tt].astype(F32)

    row0 = lax.broadcasted_iota(jnp.int32, (8, 256), 0) == 0

    def prep(j, c):
        for mm in range(2):
            w = w1f[mm] * (1.0 + gamf[mm, pl.ds(j, 1), :])
            hi = w.astype(BF16).astype(F32)
            rest = w - hi
            mid = rest.astype(BF16).astype(F32)
            low = rest - mid
            shift = jnp.where(row0, 0.5 * betf[mm, pl.ds(j, 1), :], 0.0)
            cols = jnp.concatenate([hi, mid, low, shift, jnp.zeros((DEPTH - 56, 256), F32)], axis=0)
            mat[j, HALF * mm:HALF * mm + HALF, :] = cols.T[0:HALF, :].astype(BF16)
        return c

    lax.fori_loop(0, STEPS, prep, 0)

    def product1(tile, group, half, pre, i):
        sweep0, j = item(group, half * 4 + i)
        slot = jnp.where(sweep0, STEPS + tile, j)
        pre[i] = jnp.dot(mat[j], rhs[slot], preferred_element_type=F32)

    def gelu(pre, act, i):
        for r in range(0, HIDDEN, 16):
            z = pre[i, r:r + 16, :]
            u = z * (z * z * C3 + C1)
            act[i, r:r + 16, :] = z * (1.0 + jnp.tanh(u))

    def product2(act, i):
        return (jnp.dot(w2t[0], act[i, 0:HALF, :], preferred_element_type=F32)
                + jnp.dot(w2t[1], act[i, HALF:HIDDEN, :], preferred_element_type=F32))

    def update(tile, group, half, drifts):
        for i in range(4):
            _, j = item(group, half * 4 + i)
            hrow = hs[j // 8, pl.ds(lax.rem(j, 8), 1), :]
            x = lat[tile, j] + hrow * drifts[i]
            lat[tile, j + 1] = x
            xb = x.astype(BF16)
            for r in range(3):
                rhs[j + 1, 16 * r:16 * r + 16, :] = xb

    def phase_q(tile, group, next_tile, next_group, first):
        drifts = []
        for i in range(4):
            product1(next_tile, next_group, 1, pre_b, i)
            if not first:
                drifts.append(product2(act_b, i))
            gelu(pre_a, act_a, i)
        if not first:
            update(tile, group, 1, drifts)

    def phase_p(tile, group, next_tile, next_group):
        drifts = []
        for i in range(4):
            product1(next_tile, next_group, 0, pre_a, i)
            drifts.append(product2(act_a, i))
            gelu(pre_b, act_b, i)
        update(tile, group, 0, drifts)

    for i in range(4):
        product1(0, 0, 0, pre_a, i)
    phase_q(0, 0, 0, 0, True)

    def outgoing(tile, q, pm, slot):
        return pltpu.make_async_remote_copy(
            src_ref=lat.at[tile, pl.ds(q * STEPS_DEV, STEPS_DEV)],
            dst_ref=out_ref.at[:, me * TILES + tile],
            send_sem=send_sem.at[tile, q, slot],
            recv_sem=recv_sem.at[me, tile],
            device_id={"model": pm, "time": q}, device_id_type=MESH)

    def trip(tile, group, c):
        wrap = group == GROUPS - 1
        next_tile = jnp.where(wrap, jnp.minimum(tile + 1, TILES - 1), tile)
        next_group = jnp.where(wrap, 0, group + 1)
        phase_p(tile, group, next_tile, next_group)
        phase_q(tile, group, next_tile, next_group, False)

        @pl.when(group >= GROUPS - 4)
        def _():
            q = group - (GROUPS - 4)
            outgoing(tile, q, 1 - m, 0).start()

            @pl.when(q != t)
            def _():
                outgoing(tile, q, m, 1).start()

            @pl.when(q == t)
            def _():
                for r in range(STEPS_DEV):
                    out_ref[r, me * TILES + tile] = lat[tile, q * STEPS_DEV + r]

        return c

    def tile_loop(tile, c):
        return lax.fori_loop(0, GROUPS, lambda group, cc: trip(tile, group, cc), c)

    lax.fori_loop(0, TILES, tile_loop, 0)

    def finish(i, c):
        for q in range(4):
            outgoing(i, q, 1 - m, 0).wait_send()

            @pl.when(q != t)
            def _():
                outgoing(i, q, m, 1).wait_send()

        for src in range(8):
            @pl.when(src != me)
            def _():
                pltpu.make_async_remote_copy(
                    src_ref=lat.at[0, pl.ds(0, STEPS_DEV)],
                    dst_ref=out_ref.at[:, src * TILES + i],
                    send_sem=send_sem.at[0, 0, 0],
                    recv_sem=recv_sem.at[src, i],
                    device_id={"model": m, "time": t}, device_id_type=MESH).wait_recv()
        return c

    lax.fori_loop(0, TILES, finish, 0)


def solution(mesh):
    def device_body(x_init, w_up, w_down, mod_scale, mod_shift, step_size):
        batch = x_init.shape[0]
        vmem = pl.BlockSpec(memory_space=pltpu.VMEM)
        out = pl.pallas_call(
            kernel,
            out_shape=jax.ShapeDtypeStruct((STEPS_DEV, batch, CHAN, TOKENS), F32),
            in_specs=[vmem] * 6,
            out_specs=vmem,
            scratch_shapes=[
                pltpu.VMEM((2, 4, STEPS_DEV, HALF), BF16),
                pltpu.VMEM((2, 4, STEPS_DEV, HALF), BF16),
                pltpu.VMEM((2, CHAN, HALF), BF16),
                pltpu.VMEM((2, CHAN, HALF), BF16),
                pltpu.VMEM((4, STEPS_DEV, TOKENS), F32),
                pltpu.VMEM((2, CHAN, 256), F32),
                pltpu.VMEM((2, STEPS, 256), F32),
                pltpu.VMEM((2, STEPS, 256), F32),
                pltpu.VMEM((STEPS, HIDDEN, DEPTH), BF16),
                pltpu.VMEM((2, CHAN, HALF), F32),
                pltpu.VMEM((STEPS + TILES, DEPTH, TOKENS), BF16),
                pltpu.VMEM((4, HIDDEN, TOKENS), F32),
                pltpu.VMEM((4, HIDDEN, TOKENS), F32),
                pltpu.VMEM((4, HIDDEN, TOKENS), F32),
                pltpu.VMEM((4, HIDDEN, TOKENS), F32),
                pltpu.VMEM((TILES, STEPS, CHAN, TOKENS), F32),
                pltpu.SemaphoreType.DMA((19,)),
                pltpu.SemaphoreType.DMA((19,)),
                pltpu.SemaphoreType.DMA((TILES, 4, 2)),
                pltpu.SemaphoreType.DMA((8, TILES)),
            ],
            compiler_params=pltpu.CompilerParams(
                collective_id=0, has_side_effects=True, vmem_limit_bytes=60 * 1024 * 1024),
        )(x_init.transpose(0, 2, 1), w_up, w_down.T, mod_scale, mod_shift,
          jnp.broadcast_to(step_size[:, None], (STEPS_DEV, TOKENS)))
        return out.transpose(0, 1, 3, 2)

    return jax.shard_map(
        device_body, mesh=mesh,
        in_specs=(P('data', None, None), P(None, 'model'), P('model', None), P('time', 'model'), P('time', 'model'), P('time')),
        out_specs=P('time', 'data', None, None), check_vma=False)
```

```python
import functools
import math

import jax
import jax.numpy as jnp
from jax import lax
from jax.experimental import pallas as pl
from jax.experimental.pallas import tpu as pltpu
from jax.sharding import PartitionSpec as P

MESH = pl.DeviceIdType.MESH
F32 = jnp.float32
BF16 = jnp.bfloat16

STEPS = 32
STEPS_DEV = 8
HALF = 192
HIDDEN = 384
CHAN = 16
TOKENS = 256
TILES = 8
GROUP = 8
GROUPS = 15
HALF_GROUP = GROUP // 2
DEPTH = 128

ROOT = math.sqrt(2.0 / math.pi)
C1 = 2.0 * ROOT
C3 = 8.0 * 0.044715 * ROOT


def item(group, k):
    n = group * GROUP + k
    sweep0 = n < 31
    j = jnp.where(sweep0, n, jnp.where(n < 61, n - 30, jnp.where(n < 91, n - 60, n - 89)))
    return sweep0, j


def kernel(x_ref, w1_ref, w2_ref, g_ref, b_ref, h_ref, out_ref,
           gam, bet, w1s, w2s, hs, hb, w1f, gamf, betf, mat, rhs, pre_a, pre_b, act_a, act_b, lat,
           psend, precv, send_sem, recv_sem):
    m = lax.axis_index("model")
    t = lax.axis_index("time")
    me = m * 4 + t

    offsets = [(dm, dt) for dm in range(2) for dt in range(4) if (dm, dt) != (0, 0)]
    peers = [(lax.rem(m + dm, 2), lax.rem(t + dt, 4)) for dm, dt in offsets]

    barrier = pltpu.get_barrier_semaphore()
    for pm, pt in peers:
        pl.semaphore_signal(barrier, inc=1, device_id={"model": pm, "time": pt}, device_id_type=MESH)
    pl.semaphore_wait(barrier, len(peers))

    copies = []

    def push(src, dst, peer):
        idx = len(copies)
        copy = pltpu.make_async_remote_copy(
            src_ref=src, dst_ref=dst, send_sem=psend.at[idx], recv_sem=precv.at[idx],
            device_id={"model": peer[0], "time": peer[1]}, device_id_type=MESH)
        copy.start()
        copies.append(copy)

    for (dm, dt), peer in zip(offsets, peers):
        push(g_ref, gam.at[m, t], peer)
        push(b_ref, bet.at[m, t], peer)
        if dt == 0:
            push(w1_ref, w1s.at[m], peer)
            push(w2_ref, w2s.at[m], peer)
        if dm == 0:
            push(h_ref, hs.at[t], peer)

    gam[m, t] = g_ref[...]
    bet[m, t] = b_ref[...]
    w1s[m] = w1_ref[...]
    w2s[m] = w2_ref[...]
    hs[t] = h_ref[...]
    w1f[...] = jnp.zeros_like(w1f)
    gamf[...] = jnp.zeros_like(gamf)
    betf[...] = jnp.zeros_like(betf)

    ones_zeros = jnp.concatenate([jnp.ones((16, TOKENS), BF16), jnp.zeros((DEPTH - 64, TOKENS), BF16)], axis=0)

    def init_slot(i, c):
        rhs[i, 48:DEPTH, :] = ones_zeros
        return c

    lax.fori_loop(0, STEPS + TILES, init_slot, 0)

    def init_tile(i, c):
        x0 = x_ref[me * TILES + i]
        lat[i, 0] = x0
        xb = x0.astype(BF16)
        for r in range(3):
            rhs[STEPS + i, 16 * r:16 * r + 16, :] = xb
        return c

    lax.fori_loop(0, TILES, init_tile, 0)

    for copy in copies:
        copy.wait()

    for mm in range(2):
        w1f[mm, :, 0:HALF] = w1s[mm].astype(F32) * 0.5
        for tt in range(4):
            gamf[mm, 8 * tt:8 * tt + 8, 0:HALF] = gam[mm, tt].astype(F32)
            betf[mm, 8 * tt:8 * tt + 8, 0:HALF] = bet[mm, tt].astype(F32)

    for tt in range(4):
        for r in range(STEPS_DEV):
            hb[tt * STEPS_DEV + r] = jnp.broadcast_to(hs[tt, :, r:r + 1], (CHAN, TOKENS))

    row0 = lax.broadcasted_iota(jnp.int32, (8, 256), 0) == 0

    def prep(j, c):
        for mm in range(2):
            w = w1f[mm] * (1.0 + gamf[mm, pl.ds(j, 1), :])
            hi = w.astype(BF16).astype(F32)
            rest = w - hi
            mid = rest.astype(BF16).astype(F32)
            low = rest - mid
            shift = jnp.where(row0, 0.5 * betf[mm, pl.ds(j, 1), :], 0.0)
            cols = jnp.concatenate([hi, mid, low, shift, jnp.zeros((DEPTH - 56, 256), F32)], axis=0)
            mat[j, HALF * mm:HALF * mm + HALF, :] = cols.T[0:HALF, :].astype(BF16)
        return c

    lax.fori_loop(0, STEPS, prep, 0)

    def product1(tile, group, half, pre, i):
        sweep0, j = item(group, half * HALF_GROUP + i)
        slot = jnp.where(sweep0, STEPS + tile, j)
        pre[i] = jnp.dot(mat[j], rhs[slot], preferred_element_type=F32)

    def gelu(pre, act, i):
        for r in range(0, HIDDEN, 16):
            z = pre[i, r:r + 16, :]
            u = z * (z * z * C3 + C1)
            act[i, r:r + 16, :] = (z * (1.0 + jnp.tanh(u))).astype(BF16)

    def product2(act, i):
        return (jnp.dot(w2s[0], act[i, 0:HALF, :], preferred_element_type=F32)
                + jnp.dot(w2s[1], act[i, HALF:HIDDEN, :], preferred_element_type=F32))

    def update(tile, group, drifts):
        for i in range(GROUP):
            _, j = item(group, i)
            x = lat[tile, j] + hb[j] * drifts[i]
            lat[tile, j + 1] = x
            xb = x.astype(BF16)
            for r in range(3):
                rhs[j + 1, 16 * r:16 * r + 16, :] = xb

    def phase_q(next_tile, next_group, first):
        for i in range(HALF_GROUP):
            product1(next_tile, next_group, 1, pre_b, i)
        drifts = [] if first else [product2(act_b, i) for i in range(HALF_GROUP)]
        for i in range(HALF_GROUP):
            gelu(pre_a, act_a, i)
        return drifts

    def phase_p(next_tile, next_group):
        for i in range(HALF_GROUP):
            product1(next_tile, next_group, 0, pre_a, i)
        drifts = [product2(act_a, i) for i in range(HALF_GROUP)]
        for i in range(HALF_GROUP):
            gelu(pre_b, act_b, i)
        return drifts

    for i in range(HALF_GROUP):
        product1(0, 0, 0, pre_a, i)
    phase_q(0, 0, True)

    def outgoing(tile, q, pm, slot):
        return pltpu.make_async_remote_copy(
            src_ref=lat.at[tile, pl.ds(q * STEPS_DEV, STEPS_DEV)],
            dst_ref=out_ref.at[:, me * TILES + tile],
            send_sem=send_sem.at[tile, q, slot],
            recv_sem=recv_sem.at[me, tile],
            device_id={"model": pm, "time": q}, device_id_type=MESH)

    def trip(tile, group, c):
        wrap = group == GROUPS - 1
        next_tile = jnp.where(wrap, jnp.minimum(tile + 1, TILES - 1), tile)
        next_group = jnp.where(wrap, 0, group + 1)
        drifts = phase_p(next_tile, next_group)
        drifts = drifts + phase_q(next_tile, next_group, False)
        update(tile, group, drifts)

        @pl.when(group >= GROUPS - 4)
        def _():
            q = group - (GROUPS - 4)
            outgoing(tile, q, 1 - m, 0).start()

            @pl.when(q != t)
            def _():
                outgoing(tile, q, m, 1).start()

            @pl.when(q == t)
            def _():
                for r in range(STEPS_DEV):
                    out_ref[r, me * TILES + tile] = lat[tile, q * STEPS_DEV + r]

        return c

    def tile_loop(tile, c):
        return lax.fori_loop(0, GROUPS, lambda group, cc: trip(tile, group, cc), c)

    lax.fori_loop(0, TILES, tile_loop, 0)

    def finish(i, c):
        for q in range(4):
            outgoing(i, q, 1 - m, 0).wait_send()

            @pl.when(q != t)
            def _():
                outgoing(i, q, m, 1).wait_send()

        for src in range(8):
            @pl.when(src != me)
            def _():
                pltpu.make_async_remote_copy(
                    src_ref=lat.at[0, pl.ds(0, STEPS_DEV)],
                    dst_ref=out_ref.at[:, src * TILES + i],
                    send_sem=send_sem.at[0, 0, 0],
                    recv_sem=recv_sem.at[src, i],
                    device_id={"model": m, "time": t}, device_id_type=MESH).wait_recv()
        return c

    lax.fori_loop(0, TILES, finish, 0)


def solution(mesh):
    def device_body(x_init, w_up, w_down, mod_scale, mod_shift, step_size):
        batch = x_init.shape[0]
        vmem = pl.BlockSpec(memory_space=pltpu.VMEM)
        out = pl.pallas_call(
            kernel,
            out_shape=pltpu.VMEM((STEPS_DEV, batch, CHAN, TOKENS), F32),
            in_specs=[vmem] * 6,
            out_specs=vmem,
            scratch_shapes=[
                pltpu.VMEM((2, 4, STEPS_DEV, HALF), BF16),
                pltpu.VMEM((2, 4, STEPS_DEV, HALF), BF16),
                pltpu.VMEM((2, CHAN, HALF), BF16),
                pltpu.VMEM((2, CHAN, HALF), BF16),
                pltpu.VMEM((4, 1, STEPS_DEV), F32),
                pltpu.VMEM((STEPS, CHAN, TOKENS), F32),
                pltpu.VMEM((2, CHAN, 256), F32),
                pltpu.VMEM((2, STEPS, 256), F32),
                pltpu.VMEM((2, STEPS, 256), F32),
                pltpu.VMEM((STEPS, HIDDEN, DEPTH), BF16),
                pltpu.VMEM((STEPS + TILES, DEPTH, TOKENS), BF16),
                pltpu.VMEM((HALF_GROUP, HIDDEN, TOKENS), F32),
                pltpu.VMEM((HALF_GROUP, HIDDEN, TOKENS), F32),
                pltpu.VMEM((HALF_GROUP, HIDDEN, TOKENS), BF16),
                pltpu.VMEM((HALF_GROUP, HIDDEN, TOKENS), BF16),
                pltpu.VMEM((TILES, STEPS, CHAN, TOKENS), F32),
                pltpu.SemaphoreType.DMA((19,)),
                pltpu.SemaphoreType.DMA((19,)),
                pltpu.SemaphoreType.DMA((TILES, 4, 2)),
                pltpu.SemaphoreType.DMA((8, TILES)),
            ],
            compiler_params=pltpu.CompilerParams(
                collective_id=0, has_side_effects=True, vmem_limit_bytes=24 * 1024 * 1024),
        )(x_init.transpose(0, 2, 1), w_up, w_down.T, mod_scale, mod_shift,
          step_size[None, :])
        return out.transpose(0, 1, 3, 2)

    return jax.shard_map(
        device_body, mesh=mesh,
        in_specs=(P('data', None, None), P(None, 'model'), P('model', None), P('time', 'model'), P('time', 'model'), P('time')),
        out_specs=P('time', 'data', None, None), check_vma=False)
```

```python
import functools
import math

import jax
import jax.numpy as jnp
from jax import lax
from jax.experimental import pallas as pl
from jax.experimental.pallas import tpu as pltpu
from jax.sharding import PartitionSpec as P

MESH = pl.DeviceIdType.MESH
F32 = jnp.float32
BF16 = jnp.bfloat16

STEPS = 32
STEPS_DEV = 8
HALF = 192
HIDDEN = 384
CHAN = 16
TOKENS = 256
TILES = 8
GROUP = 8
GROUPS = 15
DEPTH = 128
ORDER = ('g0 p0 p1 g1 ' 'q0 q1 p2 g2 ' 'p3 q2 q3 g3 ' 'p4 p5 g4 p6 ' 'g5 p7 g6 g7')

ROOT = math.sqrt(2.0 / math.pi)
C1 = 2.0 * ROOT
C3 = 8.0 * 0.044715 * ROOT


def item(group, k):
    n = group * GROUP + k
    sweep0 = n < 31
    j = jnp.where(sweep0, n, jnp.where(n < 61, n - 30, jnp.where(n < 91, n - 60, n - 89)))
    return sweep0, j


def kernel(x_ref, w1_ref, w2_ref, g_ref, b_ref, h_ref, out_ref,
           gam, bet, w1s, w2s, hs, hb, w1f, gamf, betf, mat, rhs, w2p, xs, pre_a, pre_b, act_a, act_b, lat,
           own_sem, psend, precv, send_sem, recv_sem):
    m = lax.axis_index("model")
    t = lax.axis_index("time")
    me = m * 4 + t

    offsets = [(dm, dt) for dm in range(2) for dt in range(4) if (dm, dt) != (0, 0)]
    peers = [(lax.rem(m + dm, 2), lax.rem(t + dt, 4)) for dm, dt in offsets]

    local = [pltpu.make_async_copy(src, dst, own_sem.at[i]) for i, (src, dst) in enumerate([
        (g_ref, gam.at[m, t]), (b_ref, bet.at[m, t]), (w1_ref, w1s.at[m]), (w2_ref, w2s.at[m]), (h_ref, hs.at[t]),
        (x_ref.at[pl.ds(me * TILES, TILES)], xs)])]
    for copy in local:
        copy.start()

    barrier = pltpu.get_barrier_semaphore()
    for pm, pt in peers:
        pl.semaphore_signal(barrier, inc=1, device_id={"model": pm, "time": pt}, device_id_type=MESH)
    pl.semaphore_wait(barrier, len(peers))

    copies = []

    def push(src, dst, peer):
        idx = len(copies)
        copy = pltpu.make_async_remote_copy(
            src_ref=src, dst_ref=dst, send_sem=psend.at[idx], recv_sem=precv.at[idx],
            device_id={"model": peer[0], "time": peer[1]}, device_id_type=MESH)
        copy.start()
        copies.append(copy)

    for (dm, dt), peer in zip(offsets, peers):
        push(g_ref, gam.at[m, t], peer)
        push(b_ref, bet.at[m, t], peer)
        if dt == 0:
            push(w1_ref, w1s.at[m], peer)
            push(w2_ref, w2s.at[m], peer)
        if dm == 0:
            push(h_ref, hs.at[t], peer)

    w1f[...] = jnp.zeros_like(w1f)
    w2p[...] = jnp.zeros_like(w2p)
    gamf[...] = jnp.zeros_like(gamf)
    betf[...] = jnp.zeros_like(betf)

    ones_zeros = jnp.concatenate([jnp.ones((16, TOKENS), BF16), jnp.zeros((DEPTH - 64, TOKENS), BF16)], axis=0)

    def init_slot(i, c):
        rhs[i, 48:DEPTH, :] = ones_zeros
        return c

    lax.fori_loop(0, STEPS + TILES, init_slot, 0)

    for copy in local:
        copy.wait()

    def init_tile(i, c):
        x0 = xs[i]
        lat[i, 0] = x0
        xb = x0.astype(BF16)
        for r in range(3):
            rhs[STEPS + i, 16 * r:16 * r + 16, :] = xb
        return c

    lax.fori_loop(0, TILES, init_tile, 0)

    for copy in copies:
        copy.wait()

    for mm in range(2):
        w1f[mm, :, 0:HALF] = w1s[mm].astype(F32) * 0.5
        for u in range(2):
            w2p[CHAN * u:CHAN * u + CHAN, 256 * u + 128 * mm:256 * u + 128 * mm + 128] = w2s[mm][:, 0:128]
        for tt in range(4):
            gamf[mm, 8 * tt:8 * tt + 8, 0:HALF] = gam[mm, tt].astype(F32)
            betf[mm, 8 * tt:8 * tt + 8, 0:HALF] = bet[mm, tt].astype(F32)

    for tt in range(4):
        for r in range(STEPS_DEV):
            hb[tt * STEPS_DEV + r] = jnp.broadcast_to(hs[tt, :, r:r + 1], (CHAN, TOKENS))

    tails = jnp.concatenate([w2s[mm].astype(F32)[:, 128:HALF] for mm in range(2)], axis=1).astype(BF16)
    for u in range(2):
        w2p[CHAN * u:CHAN * u + CHAN, 512 + 128 * u:640 + 128 * u] = tails

    row0 = lax.broadcasted_iota(jnp.int32, (8, 256), 0) == 0

    def prep(j, c):
        for mm in range(2):
            w = w1f[mm] * (1.0 + gamf[mm, pl.ds(j, 1), :])
            hi = w.astype(BF16).astype(F32)
            rest = w - hi
            mid = rest.astype(BF16).astype(F32)
            low = rest - mid
            shift = jnp.where(row0, 0.5 * betf[mm, pl.ds(j, 1), :], 0.0)
            cols = jnp.concatenate([hi, mid, low, shift, jnp.zeros((DEPTH - 56, 256), F32)], axis=0)
            mat[j, HALF * mm:HALF * mm + HALF, :] = cols.T[0:HALF, :].astype(BF16)
        return c

    lax.fori_loop(0, STEPS, prep, 0)

    def product1(tile, group, pre, i):
        sweep0, j = item(group, i)
        slot = jnp.where(sweep0, STEPS + tile, j)
        pre[i] = jnp.dot(mat[j], rhs[slot], preferred_element_type=F32)

    def gelu(pre, act, i):
        u = i % 2
        for r in range(0, HIDDEN, 16):
            part, k = r // HALF, r % HALF
            row = u * 256 + part * 128 + k if k < 128 else 512 + u * 128 + part * 64 + k - 128
            z = pre[i, r:r + 16, :]
            f = z * (z * z * C3 + C1)
            act[i // 2, row:row + 16, :] = (z * (1.0 + jnp.tanh(f))).astype(BF16)

    def product2(act, pair):
        both = jnp.dot(w2p[...], act[pair], preferred_element_type=F32)
        return [both[0:CHAN], both[CHAN:2 * CHAN]]

    def update(tile, group, drifts):
        for i in range(GROUP):
            _, j = item(group, i)
            x = lat[tile, j] + hb[j] * drifts[i]
            lat[tile, j + 1] = x
            xb = x.astype(BF16)
            slot = jnp.where(tile == TILES, STEPS + TILES, j + 1)
            for r in range(3):
                rhs[slot, 16 * r:16 * r + 16, :] = xb

    pres, acts = [pre_a, pre_b], [act_a, act_b]

    def split(index):
        return lax.div(index, GROUPS), lax.rem(index, GROUPS)

    def second_products(act):
        return [d for i in range(GROUP // 2) for d in product2(act, i)]

    def stage(index, parity):
        next_tile, next_group = split(jnp.minimum(index + 1, TILES * GROUPS - 1))
        drifts = []
        for step in ORDER.split():
            kind, i = step[0], int(step[1])
            if kind == 'g':
                gelu(pres[parity], acts[parity], i)
            elif kind == 'p':
                product1(next_tile, next_group, pres[1 - parity], i)
            else:
                drifts += product2(acts[1 - parity], i)
        tile, group = split(jnp.maximum(index - 1, 0))
        update(jnp.where(index == 0, TILES, tile), group, drifts)

    for i in range(GROUP):
        product1(0, 0, pre_a, i)

    def outgoing(tile, q, pm, slot):
        return pltpu.make_async_remote_copy(
            src_ref=lat.at[tile, pl.ds(q * STEPS_DEV, STEPS_DEV)],
            dst_ref=out_ref.at[:, me * TILES + tile],
            send_sem=send_sem.at[tile, q, slot],
            recv_sem=recv_sem.at[me, tile],
            device_id={"model": pm, "time": q}, device_id_type=MESH)

    def send(tile, q):
        outgoing(tile, q, 1 - m, 0).start()

        @pl.when(q != t)
        def _():
            outgoing(tile, q, m, 1).start()

        @pl.when(q == t)
        def _():
            for r in range(STEPS_DEV):
                out_ref[r, me * TILES + tile] = lat[tile, q * STEPS_DEV + r]

    def send_done(index):
        tile, group = split(jnp.maximum(index - 1, 0))

        @pl.when(group >= GROUPS - 4)
        def _():
            send(tile, group - (GROUPS - 4))

    def trip(i, c):
        for parity in range(2):
            stage(2 * i + parity, parity)
            send_done(2 * i + parity)
        return c

    lax.fori_loop(0, TILES * GROUPS // 2, trip, 0)
    update(TILES - 1, GROUPS - 1, second_products(act_b))
    send(TILES - 1, 3)

    def finish(i, c):
        for q in range(4):
            outgoing(i, q, 1 - m, 0).wait_send()

            @pl.when(q != t)
            def _():
                outgoing(i, q, m, 1).wait_send()

        for src in range(8):
            @pl.when(src != me)
            def _():
                pltpu.make_async_remote_copy(
                    src_ref=lat.at[0, pl.ds(0, STEPS_DEV)],
                    dst_ref=out_ref.at[:, src * TILES + i],
                    send_sem=send_sem.at[0, 0, 0],
                    recv_sem=recv_sem.at[src, i],
                    device_id={"model": m, "time": t}, device_id_type=MESH).wait_recv()
        return c

    lax.fori_loop(0, TILES, finish, 0)


def solution(mesh):
    def device_body(x_init, w_up, w_down, mod_scale, mod_shift, step_size):
        batch = x_init.shape[0]
        vmem = pl.BlockSpec(memory_space=pltpu.VMEM)
        hbm = pl.BlockSpec(memory_space=pltpu.HBM)
        out = pl.pallas_call(
            kernel,
            out_shape=pltpu.VMEM((STEPS_DEV, batch, CHAN, TOKENS), F32),
            in_specs=[hbm] * 6,
            out_specs=vmem,
            scratch_shapes=[
                pltpu.VMEM((2, 4, STEPS_DEV, HALF), BF16),
                pltpu.VMEM((2, 4, STEPS_DEV, HALF), BF16),
                pltpu.VMEM((2, CHAN, HALF), BF16),
                pltpu.VMEM((2, CHAN, HALF), BF16),
                pltpu.VMEM((4, 1, STEPS_DEV), F32),
                pltpu.VMEM((STEPS, CHAN, TOKENS), F32),
                pltpu.VMEM((2, CHAN, 256), F32),
                pltpu.VMEM((2, STEPS, 256), F32),
                pltpu.VMEM((2, STEPS, 256), F32),
                pltpu.VMEM((STEPS, HIDDEN, DEPTH), BF16),
                pltpu.VMEM((STEPS + TILES + 1, DEPTH, TOKENS), BF16),
                pltpu.VMEM((2 * CHAN, 2 * HIDDEN), BF16),
                pltpu.VMEM((TILES, CHAN, TOKENS), F32),
                pltpu.VMEM((GROUP, HIDDEN, TOKENS), F32),
                pltpu.VMEM((GROUP, HIDDEN, TOKENS), F32),
                pltpu.VMEM((GROUP // 2, 2 * HIDDEN, TOKENS), BF16),
                pltpu.VMEM((GROUP // 2, 2 * HIDDEN, TOKENS), BF16),
                pltpu.VMEM((TILES + 1, STEPS, CHAN, TOKENS), F32),
                pltpu.SemaphoreType.DMA((6,)),
                pltpu.SemaphoreType.DMA((19,)),
                pltpu.SemaphoreType.DMA((19,)),
                pltpu.SemaphoreType.DMA((TILES, 4, 2)),
                pltpu.SemaphoreType.DMA((8, TILES)),
            ],
            compiler_params=pltpu.CompilerParams(
                collective_id=0, has_side_effects=True, vmem_limit_bytes=32 * 1024 * 1024),
        )(*[pltpu.with_memory_space_constraint(a, pltpu.HBM) for a in (
            x_init.transpose(0, 2, 1), w_up, w_down.T, mod_scale, mod_shift, step_size[None, :])])
        return out.transpose(0, 1, 3, 2)

    return jax.shard_map(
        device_body, mesh=mesh,
        in_specs=(P('data', None, None), P(None, 'model'), P('model', None), P('time', 'model'), P('time', 'model'), P('time')),
        out_specs=P('time', 'data', None, None), check_vma=False)
```

```python
import functools
import math

import jax
import jax.numpy as jnp
from jax import lax
from jax.experimental import pallas as pl
from jax.experimental.pallas import tpu as pltpu
from jax.sharding import PartitionSpec as P

MESH = pl.DeviceIdType.MESH
F32 = jnp.float32
BF16 = jnp.bfloat16

STEPS = 32
STEPS_DEV = 8
HALF = 192
HIDDEN = 384
CHAN = 16
TOKENS = 256
TILES = 8
GROUP = 8
ITEMS = 118
GROUPS = TILES * ITEMS // GROUP
DEPTH = 128
PARTS = 2
PART = HIDDEN // PARTS
ORDER = (
    ('g', 0), ('p', 0), ('g', 1), ('p', 1), ('q', 0), ('g', 2), ('p', 2), ('g', 3), ('p', 3), ('q', 1),
    ('g', 4), ('p', 4), ('g', 5), ('p', 5), ('q', 2), ('g', 6), ('p', 6), ('g', 7), ('p', 7), ('q', 3),
    ('g', 8), ('p', 8), ('g', 9), ('p', 9), ('g', 10), ('p', 10), ('g', 11), ('p', 11), ('g', 12), ('p', 12),
    ('g', 13), ('p', 13), ('g', 14), ('p', 14), ('p', 15), ('g', 15),
)

ROOT = math.sqrt(2.0 / math.pi)
C1 = 2.0 * ROOT
C3 = 8.0 * 0.044715 * ROOT


def item(group, k):
    start = group * GROUP
    tile, n = lax.div(start, ITEMS), lax.rem(start, ITEMS) + k
    wrap = n >= ITEMS
    tile, n = jnp.where(wrap, tile + 1, tile), jnp.where(wrap, n - ITEMS, n)
    j = jnp.where(n < 31, n, jnp.where(n < 61, n - 30, jnp.where(n < 90, n - 59, n - 87)))
    return tile, n < 31, j


def kernel(x_ref, w1_ref, w2_ref, g_ref, b_ref, h_ref, out_ref,
           gam, bet, w1s, w2s, hs, hb, w1f, gamf, betf, mat, rhs, w2p, xs, pre_a, pre_b, act_a, act_b, lat,
           own_sem, psend, precv, send_sem, recv_sem):
    m = lax.axis_index("model")
    t = lax.axis_index("time")
    me = m * 4 + t

    offsets = [(dm, dt) for dm in range(2) for dt in range(4) if (dm, dt) != (0, 0)]
    peers = [(lax.rem(m + dm, 2), lax.rem(t + dt, 4)) for dm, dt in offsets]

    local = [pltpu.make_async_copy(src, dst, own_sem.at[i]) for i, (src, dst) in enumerate([
        (g_ref, gam.at[m, t]), (b_ref, bet.at[m, t]), (w1_ref, w1s.at[m]), (w2_ref, w2s.at[m]), (h_ref, hs.at[t]),
        (x_ref.at[pl.ds(me * TILES, TILES)], xs)])]
    for copy in local:
        copy.start()

    barrier = pltpu.get_barrier_semaphore()
    for pm, pt in peers:
        pl.semaphore_signal(barrier, inc=1, device_id={"model": pm, "time": pt}, device_id_type=MESH)
    pl.semaphore_wait(barrier, len(peers))

    copies = []

    def push(src, dst, peer):
        idx = len(copies)
        copy = pltpu.make_async_remote_copy(
            src_ref=src, dst_ref=dst, send_sem=psend.at[idx], recv_sem=precv.at[idx],
            device_id={"model": peer[0], "time": peer[1]}, device_id_type=MESH)
        copy.start()
        copies.append(copy)

    for (dm, dt), peer in zip(offsets, peers):
        push(g_ref, gam.at[m, t], peer)
        push(b_ref, bet.at[m, t], peer)
        if dt == 0:
            push(w1_ref, w1s.at[m], peer)
            push(w2_ref, w2s.at[m], peer)
        if dm == 0:
            push(h_ref, hs.at[t], peer)

    w1f[...] = jnp.zeros_like(w1f)
    w2p[...] = jnp.zeros_like(w2p)
    gamf[...] = jnp.zeros_like(gamf)
    betf[...] = jnp.zeros_like(betf)

    ones_zeros = jnp.concatenate([jnp.ones((16, TOKENS), BF16), jnp.zeros((DEPTH - 64, TOKENS), BF16)], axis=0)

    def init_slot(i, c):
        rhs[i, 48:DEPTH, :] = ones_zeros
        return c

    lax.fori_loop(0, STEPS + TILES, init_slot, 0)

    for copy in local:
        copy.wait()

    def init_tile(i, c):
        x0 = xs[i]
        lat[i, 0] = x0
        xb = x0.astype(BF16)
        for r in range(3):
            rhs[STEPS + i, 16 * r:16 * r + 16, :] = xb
        return c

    lax.fori_loop(0, TILES, init_tile, 0)

    for copy in copies:
        copy.wait()

    for mm in range(2):
        w1f[mm, :, 0:HALF] = w1s[mm].astype(F32) * 0.5
        for u in range(2):
            w2p[CHAN * u:CHAN * u + CHAN, 256 * u + 128 * mm:256 * u + 128 * mm + 128] = w2s[mm][:, 0:128]
        for tt in range(4):
            gamf[mm, 8 * tt:8 * tt + 8, 0:HALF] = gam[mm, tt].astype(F32)
            betf[mm, 8 * tt:8 * tt + 8, 0:HALF] = bet[mm, tt].astype(F32)

    for tt in range(4):
        for r in range(STEPS_DEV):
            hb[tt * STEPS_DEV + r] = jnp.broadcast_to(hs[tt, :, r:r + 1], (CHAN, TOKENS))

    tails = jnp.concatenate([w2s[mm].astype(F32)[:, 128:HALF] for mm in range(2)], axis=1).astype(BF16)
    for u in range(2):
        w2p[CHAN * u:CHAN * u + CHAN, 512 + 128 * u:640 + 128 * u] = tails

    row0 = lax.broadcasted_iota(jnp.int32, (8, 256), 0) == 0

    def prep(j, c):
        for mm in range(2):
            w = w1f[mm] * (1.0 + gamf[mm, pl.ds(j, 1), :])
            hi = w.astype(BF16).astype(F32)
            rest = w - hi
            mid = rest.astype(BF16).astype(F32)
            low = rest - mid
            shift = jnp.where(row0, 0.5 * betf[mm, pl.ds(j, 1), :], 0.0)
            cols = jnp.concatenate([hi, mid, low, shift, jnp.zeros((DEPTH - 56, 256), F32)], axis=0)
            mat[j, HALF * mm:HALF * mm + HALF, :] = cols.T[0:HALF, :].astype(BF16)
        return c

    lax.fori_loop(0, STEPS, prep, 0, unroll=4)

    def product1(group, pre, h):
        i, rows = h // PARTS, pl.ds(h % PARTS * PART, PART)
        tile, sweep0, j = item(group, i)
        slot = jnp.where(sweep0, STEPS + tile, j)
        pre[i, rows, :] = jnp.dot(mat[j, rows, :], rhs[slot], preferred_element_type=F32)

    def gelu(pre, act, h):
        i = h // PARTS
        u = i % 2
        for r in range(h % PARTS * PART, h % PARTS * PART + PART, 16):
            part, k = r // HALF, r % HALF
            row = u * 256 + part * 128 + k if k < 128 else 512 + u * 128 + part * 64 + k - 128
            z = pre[i, r:r + 16, :]
            f = z * (z * z * C3 + C1)
            act[i // 2, row:row + 16, :] = (z * (1.0 + jnp.tanh(f))).astype(BF16)

    def product2(act, pair):
        both = jnp.dot(w2p[...], act[pair], preferred_element_type=F32)
        return [both[0:CHAN], both[CHAN:2 * CHAN]]

    def update(group, spare, drifts):
        for i in range(GROUP):
            tile, _, j = item(group, i)
            tile = jnp.where(spare, TILES, tile)
            x = lat[tile, j] + hb[j] * drifts[i]
            lat[tile, j + 1] = x
            xb = x.astype(BF16)
            slot = jnp.where(spare, STEPS + TILES, j + 1)
            for r in range(3):
                rhs[slot, 16 * r:16 * r + 16, :] = xb

    pres, acts = [pre_a, pre_b], [act_a, act_b]

    def second_products(act):
        return [d for i in range(GROUP // 2) for d in product2(act, i)]

    def stage(index, parity):
        following = jnp.minimum(index + 1, GROUPS - 1)
        drifts = []
        for kind, i in ORDER:
            if kind == 'g':
                gelu(pres[parity], acts[parity], i)
            elif kind == 'p':
                product1(following, pres[1 - parity], i)
            else:
                drifts += product2(acts[1 - parity], i)
        update(jnp.maximum(index - 1, 0), index == 0, drifts)

    for h in range(PARTS * GROUP):
        product1(0, pre_a, h)

    def outgoing(tile, q, pm, slot):
        return pltpu.make_async_remote_copy(
            src_ref=lat.at[tile, pl.ds(q * STEPS_DEV, STEPS_DEV)],
            dst_ref=out_ref.at[:, me * TILES + tile],
            send_sem=send_sem.at[q, slot],
            recv_sem=recv_sem.at[me],
            device_id={"model": pm, "time": q}, device_id_type=MESH)

    def send(tile, q):
        outgoing(tile, q, 1 - m, 0).start()

        @pl.when(q != t)
        def _():
            outgoing(tile, q, m, 1).start()

        @pl.when(q == t)
        def _():
            for r in range(STEPS_DEV):
                out_ref[r, me * TILES + tile] = lat[tile, q * STEPS_DEV + r]

    def send_done(group):
        past = jnp.maximum(group * GROUP + GROUP - 1 - 93, 0)
        tile, rest = lax.div(past, ITEMS), lax.rem(past, ITEMS)

        @pl.when((group * GROUP + GROUP - 1 >= 93) & (rest < 32))
        def _():
            send(tile, lax.div(rest, 8))

    def trip(i, c):
        for parity in range(2):
            stage(2 * i + parity, parity)
            send_done(2 * i + parity - 1)
        return c

    lax.fori_loop(0, GROUPS // 2, trip, 0)
    update(GROUPS - 1, False, second_products(act_b))
    send(TILES - 1, 3)

    def waiter(q, slot, src):
        return pltpu.make_async_remote_copy(
            src_ref=lat.at[pl.ds(0, TILES), pl.ds(q * STEPS_DEV, STEPS_DEV)],
            dst_ref=out_ref.at[:, pl.ds(src * TILES, TILES)],
            send_sem=send_sem.at[q, slot],
            recv_sem=recv_sem.at[src],
            device_id={"model": 1 - m, "time": t}, device_id_type=MESH)

    for q in range(4):
        waiter(q, 0, 0).wait_send()

        @pl.when(q != t)
        def _():
            waiter(q, 1, 0).wait_send()

    for src in range(8):
        @pl.when(src != me)
        def _():
            waiter(0, 0, src).wait_recv()


def solution(mesh):
    def device_body(x_init, w_up, w_down, mod_scale, mod_shift, step_size):
        batch = x_init.shape[0]
        vmem = pl.BlockSpec(memory_space=pltpu.VMEM)
        hbm = pl.BlockSpec(memory_space=pltpu.HBM)
        out = pl.pallas_call(
            kernel,
            out_shape=pltpu.VMEM((STEPS_DEV, batch, CHAN, TOKENS), F32),
            in_specs=[hbm] * 6,
            out_specs=vmem,
            scratch_shapes=[
                pltpu.VMEM((2, 4, STEPS_DEV, HALF), BF16),
                pltpu.VMEM((2, 4, STEPS_DEV, HALF), BF16),
                pltpu.VMEM((2, CHAN, HALF), BF16),
                pltpu.VMEM((2, CHAN, HALF), BF16),
                pltpu.VMEM((4, 1, STEPS_DEV), F32),
                pltpu.VMEM((STEPS, CHAN, TOKENS), F32),
                pltpu.VMEM((2, CHAN, 256), F32),
                pltpu.VMEM((2, STEPS, 256), F32),
                pltpu.VMEM((2, STEPS, 256), F32),
                pltpu.VMEM((STEPS, HIDDEN, DEPTH), BF16),
                pltpu.VMEM((STEPS + TILES + 1, DEPTH, TOKENS), BF16),
                pltpu.VMEM((2 * CHAN, 2 * HIDDEN), BF16),
                pltpu.VMEM((TILES, CHAN, TOKENS), F32),
                pltpu.VMEM((GROUP, HIDDEN, TOKENS), F32),
                pltpu.VMEM((GROUP, HIDDEN, TOKENS), F32),
                pltpu.VMEM((GROUP // 2, 2 * HIDDEN, TOKENS), BF16),
                pltpu.VMEM((GROUP // 2, 2 * HIDDEN, TOKENS), BF16),
                pltpu.VMEM((TILES + 1, STEPS, CHAN, TOKENS), F32),
                pltpu.SemaphoreType.DMA((6,)),
                pltpu.SemaphoreType.DMA((19,)),
                pltpu.SemaphoreType.DMA((19,)),
                pltpu.SemaphoreType.DMA((4, 2)),
                pltpu.SemaphoreType.DMA((8,)),
            ],
            compiler_params=pltpu.CompilerParams(
                collective_id=0, has_side_effects=True, vmem_limit_bytes=32 * 1024 * 1024),
        )(*[pltpu.with_memory_space_constraint(a, pltpu.HBM) for a in (
            x_init.transpose(0, 2, 1), w_up, w_down.T, mod_scale, mod_shift, step_size[None, :])])
        return out.transpose(0, 1, 3, 2)

    return jax.shard_map(
        device_body, mesh=mesh,
        in_specs=(P('data', None, None), P(None, 'model'), P('model', None), P('time', 'model'), P('time', 'model'), P('time')),
        out_specs=P('time', 'data', None, None), check_vma=False)
```

```python
import functools
import math

import jax
import jax.numpy as jnp
from jax import lax
from jax.experimental import pallas as pl
from jax.experimental.pallas import tpu as pltpu
from jax.sharding import PartitionSpec as P

MESH = pl.DeviceIdType.MESH
F32 = jnp.float32
BF16 = jnp.bfloat16

STEPS = 32
STEPS_DEV = 8
HALF = 192
HIDDEN = 384
CHAN = 16
TOKENS = 256
TILES = 8
GROUP = 8
ITEMS = 118
GROUPS = TILES * ITEMS // GROUP
DEPTH = 128
PARTS = 2
PART = HIDDEN // PARTS
ORDER = (
    ('g', 0), ('p', 0), ('q', 0), ('g', 1), ('p', 1), ('p', 2), ('g', 2), ('p', 3), ('g', 3), ('q', 1),
    ('p', 4), ('g', 4), ('p', 5), ('g', 5), ('p', 6), ('q', 2), ('g', 6), ('p', 7), ('g', 7), ('p', 8),
    ('g', 8), ('q', 3), ('p', 9), ('g', 9), ('p', 10), ('g', 10), ('p', 11), ('g', 11), ('p', 12), ('g', 12),
    ('p', 13), ('g', 13), ('p', 14), ('g', 14), ('p', 15), ('g', 15),
)

ROOT = math.sqrt(2.0 / math.pi)
C1 = 2.0 * ROOT
C3 = 8.0 * 0.044715 * ROOT


def item(group, k):
    start = group * GROUP
    tile, n = lax.div(start, ITEMS), lax.rem(start, ITEMS) + k
    wrap = n >= ITEMS
    tile, n = jnp.where(wrap, tile + 1, tile), jnp.where(wrap, n - ITEMS, n)
    j = jnp.where(n < 31, n, jnp.where(n < 61, n - 30, jnp.where(n < 90, n - 59, n - 87)))
    return tile, n < 31, j


def kernel(x_ref, w1_ref, w2_ref, g_ref, b_ref, h_ref, out_ref,
           gam, bet, w1s, w2s, hs, hb, w1f, gamf, betf, mat, rhs, w2p, xs, pre_a, pre_b, act_a, act_b, lat,
           own_sem, psend, precv, send_sem, recv_sem):
    m = lax.axis_index("model")
    t = lax.axis_index("time")
    me = m * 4 + t

    offsets = [(dm, dt) for dm in range(2) for dt in range(4) if (dm, dt) != (0, 0)]
    peers = [(lax.rem(m + dm, 2), lax.rem(t + dt, 4)) for dm, dt in offsets]

    local = [pltpu.make_async_copy(src, dst, own_sem.at[i]) for i, (src, dst) in enumerate([
        (g_ref, gam.at[m, t]), (b_ref, bet.at[m, t]), (w1_ref, w1s.at[m]), (w2_ref, w2s.at[m]), (h_ref, hs.at[t]),
        (x_ref.at[pl.ds(me * TILES, TILES)], xs)])]
    for copy in local:
        copy.start()

    barrier = pltpu.get_barrier_semaphore()
    for pm, pt in peers:
        pl.semaphore_signal(barrier, inc=1, device_id={"model": pm, "time": pt}, device_id_type=MESH)
    pl.semaphore_wait(barrier, len(peers))

    copies = []

    def push(src, dst, peer):
        idx = len(copies)
        copy = pltpu.make_async_remote_copy(
            src_ref=src, dst_ref=dst, send_sem=psend.at[idx], recv_sem=precv.at[idx],
            device_id={"model": peer[0], "time": peer[1]}, device_id_type=MESH)
        copy.start()
        copies.append(copy)

    for (dm, dt), peer in zip(offsets, peers):
        push(g_ref, gam.at[m, t], peer)
        push(b_ref, bet.at[m, t], peer)
        if dt == 0:
            push(w1_ref, w1s.at[m], peer)
            push(w2_ref, w2s.at[m], peer)
        if dm == 0:
            push(h_ref, hs.at[t], peer)

    w1f[...] = jnp.zeros_like(w1f)
    w2p[...] = jnp.zeros_like(w2p)
    gamf[...] = jnp.zeros_like(gamf)
    betf[...] = jnp.zeros_like(betf)

    ones_zeros = jnp.concatenate([jnp.ones((16, TOKENS), BF16), jnp.zeros((DEPTH - 64, TOKENS), BF16)], axis=0)

    def init_slot(i, c):
        rhs[i, 48:DEPTH, :] = ones_zeros
        return c

    lax.fori_loop(0, STEPS + TILES, init_slot, 0)

    for copy in local:
        copy.wait()

    def init_tile(i, c):
        x0 = xs[i]
        lat[i, 0] = x0
        xb = x0.astype(BF16)
        for r in range(3):
            rhs[STEPS + i, 16 * r:16 * r + 16, :] = xb
        return c

    lax.fori_loop(0, TILES, init_tile, 0)

    for copy in copies:
        copy.wait()

    for mm in range(2):
        w1f[mm, :, 0:HALF] = w1s[mm].astype(F32) * 0.5
        for u in range(2):
            w2p[CHAN * u:CHAN * u + CHAN, 256 * u + 128 * mm:256 * u + 128 * mm + 128] = w2s[mm][:, 0:128]
        for tt in range(4):
            gamf[mm, 8 * tt:8 * tt + 8, 0:HALF] = gam[mm, tt].astype(F32)
            betf[mm, 8 * tt:8 * tt + 8, 0:HALF] = bet[mm, tt].astype(F32)

    for tt in range(4):
        for r in range(STEPS_DEV):
            hb[tt * STEPS_DEV + r] = jnp.broadcast_to(hs[tt, :, r:r + 1], (CHAN, TOKENS))

    tails = jnp.concatenate([w2s[mm].astype(F32)[:, 128:HALF] for mm in range(2)], axis=1).astype(BF16)
    for u in range(2):
        w2p[CHAN * u:CHAN * u + CHAN, 512 + 128 * u:640 + 128 * u] = tails

    row0 = lax.broadcasted_iota(jnp.int32, (8, 256), 0) == 0

    def prep(j, c):
        for mm in range(2):
            w = w1f[mm] * (1.0 + gamf[mm, pl.ds(j, 1), :])
            hi = w.astype(BF16).astype(F32)
            rest = w - hi
            mid = rest.astype(BF16).astype(F32)
            low = rest - mid
            shift = jnp.where(row0, 0.5 * betf[mm, pl.ds(j, 1), :], 0.0)
            cols = jnp.concatenate([hi, mid, low, shift, jnp.zeros((DEPTH - 56, 256), F32)], axis=0)
            mat[j, HALF * mm:HALF * mm + HALF, :] = cols.T[0:HALF, :].astype(BF16)
        return c

    lax.fori_loop(0, STEPS, prep, 0, unroll=4)

    def product1(group, pre, h):
        i, rows = h // PARTS, pl.ds(h % PARTS * PART, PART)
        tile, sweep0, j = item(group, i)
        slot = jnp.where(sweep0, STEPS + tile, j)
        pre[i, rows, :] = jnp.dot(mat[j, rows, :], rhs[slot], preferred_element_type=F32)

    def gelu(pre, act, h):
        i = h // PARTS
        u = i % 2
        for r in range(h % PARTS * PART, h % PARTS * PART + PART, 16):
            part, k = r // HALF, r % HALF
            row = u * 256 + part * 128 + k if k < 128 else 512 + u * 128 + part * 64 + k - 128
            z = pre[i, r:r + 16, :]
            f = z * (z * z * C3 + C1)
            act[i // 2, row:row + 16, :] = (z * (1.0 + jnp.tanh(f))).astype(BF16)

    def product2(act, pair):
        both = jnp.dot(w2p[...], act[pair], preferred_element_type=F32)
        return [both[0:CHAN], both[CHAN:2 * CHAN]]

    def update(group, spare, drifts):
        for i in range(GROUP):
            tile, _, j = item(group, i)
            tile = jnp.where(spare, TILES, tile)
            x = lat[tile, j] + hb[j] * drifts[i]
            lat[tile, j + 1] = x
            xb = x.astype(BF16)
            slot = jnp.where(spare, STEPS + TILES, j + 1)
            for r in range(3):
                rhs[slot, 16 * r:16 * r + 16, :] = xb

    pres, acts = [pre_a, pre_b], [act_a, act_b]

    def second_products(act):
        return [d for i in range(GROUP // 2) for d in product2(act, i)]

    def stage(index, parity):
        following = jnp.minimum(index + 1, GROUPS - 1)
        drifts = []
        for kind, i in ORDER:
            if kind == 'g':
                gelu(pres[parity], acts[parity], i)
            elif kind == 'p':
                product1(following, pres[1 - parity], i)
            else:
                drifts += product2(acts[1 - parity], i)
        update(jnp.maximum(index - 1, 0), index == 0, drifts)

    for h in range(PARTS * GROUP):
        product1(0, pre_a, h)

    def outgoing(tile, q, pm, slot):
        return pltpu.make_async_remote_copy(
            src_ref=lat.at[tile, pl.ds(q * STEPS_DEV, STEPS_DEV)],
            dst_ref=out_ref.at[:, me * TILES + tile],
            send_sem=send_sem.at[q, slot],
            recv_sem=recv_sem.at[me],
            device_id={"model": pm, "time": q}, device_id_type=MESH)

    def send(tile, q):
        outgoing(tile, q, 1 - m, 0).start()

        @pl.when(q != t)
        def _():
            outgoing(tile, q, m, 1).start()

        @pl.when(q == t)
        def _():
            for r in range(STEPS_DEV):
                out_ref[r, me * TILES + tile] = lat[tile, q * STEPS_DEV + r]

    def send_done(group):
        past = jnp.maximum(group * GROUP + GROUP - 1 - 93, 0)
        tile, rest = lax.div(past, ITEMS), lax.rem(past, ITEMS)

        @pl.when((group * GROUP + GROUP - 1 >= 93) & (rest < 32))
        def _():
            send(tile, lax.div(rest, 8))

    def trip(i, c):
        for parity in range(2):
            stage(2 * i + parity, parity)
            send_done(2 * i + parity - 1)
        return c

    lax.fori_loop(0, GROUPS // 2, trip, 0)
    update(GROUPS - 1, False, second_products(act_b))
    send(TILES - 1, 3)

    def waiter(q, slot, src):
        return pltpu.make_async_remote_copy(
            src_ref=lat.at[pl.ds(0, TILES), pl.ds(q * STEPS_DEV, STEPS_DEV)],
            dst_ref=out_ref.at[:, pl.ds(src * TILES, TILES)],
            send_sem=send_sem.at[q, slot],
            recv_sem=recv_sem.at[src],
            device_id={"model": 1 - m, "time": t}, device_id_type=MESH)

    for q in range(4):
        waiter(q, 0, 0).wait_send()

        @pl.when(q != t)
        def _():
            waiter(q, 1, 0).wait_send()

    for src in range(8):
        @pl.when(src != me)
        def _():
            waiter(0, 0, src).wait_recv()


def solution(mesh):
    def device_body(x_init, w_up, w_down, mod_scale, mod_shift, step_size):
        batch = x_init.shape[0]
        vmem = pl.BlockSpec(memory_space=pltpu.VMEM)
        hbm = pl.BlockSpec(memory_space=pltpu.HBM)
        out = pl.pallas_call(
            kernel,
            out_shape=pltpu.VMEM((STEPS_DEV, batch, CHAN, TOKENS), F32),
            in_specs=[hbm] * 6,
            out_specs=vmem,
            scratch_shapes=[
                pltpu.VMEM((2, 4, STEPS_DEV, HALF), BF16),
                pltpu.VMEM((2, 4, STEPS_DEV, HALF), BF16),
                pltpu.VMEM((2, CHAN, HALF), BF16),
                pltpu.VMEM((2, CHAN, HALF), BF16),
                pltpu.VMEM((4, 1, STEPS_DEV), F32),
                pltpu.VMEM((STEPS, CHAN, TOKENS), F32),
                pltpu.VMEM((2, CHAN, 256), F32),
                pltpu.VMEM((2, STEPS, 256), F32),
                pltpu.VMEM((2, STEPS, 256), F32),
                pltpu.VMEM((STEPS, HIDDEN, DEPTH), BF16),
                pltpu.VMEM((STEPS + TILES + 1, DEPTH, TOKENS), BF16),
                pltpu.VMEM((2 * CHAN, 2 * HIDDEN), BF16),
                pltpu.VMEM((TILES, CHAN, TOKENS), F32),
                pltpu.VMEM((GROUP, HIDDEN, TOKENS), F32),
                pltpu.VMEM((GROUP, HIDDEN, TOKENS), F32),
                pltpu.VMEM((GROUP // 2, 2 * HIDDEN, TOKENS), BF16),
                pltpu.VMEM((GROUP // 2, 2 * HIDDEN, TOKENS), BF16),
                pltpu.VMEM((TILES + 1, STEPS, CHAN, TOKENS), F32),
                pltpu.SemaphoreType.DMA((6,)),
                pltpu.SemaphoreType.DMA((19,)),
                pltpu.SemaphoreType.DMA((19,)),
                pltpu.SemaphoreType.DMA((4, 2)),
                pltpu.SemaphoreType.DMA((8,)),
            ],
            compiler_params=pltpu.CompilerParams(
                collective_id=0, has_side_effects=True, vmem_limit_bytes=32 * 1024 * 1024),
        )(*[pltpu.with_memory_space_constraint(a, pltpu.HBM) for a in (
            x_init.transpose(0, 2, 1), w_up, w_down.T, mod_scale, mod_shift, step_size[None, :])])
        return out.transpose(0, 1, 3, 2)

    return jax.shard_map(
        device_body, mesh=mesh,
        in_specs=(P('data', None, None), P(None, 'model'), P('model', None), P('time', 'model'), P('time', 'model'), P('time')),
        out_specs=P('time', 'data', None, None), check_vma=False)
```

```python
import functools
import math

import jax
import jax.numpy as jnp
from jax import lax
from jax.experimental import pallas as pl
from jax.experimental.pallas import tpu as pltpu
from jax.sharding import PartitionSpec as P

MESH = pl.DeviceIdType.MESH
F32 = jnp.float32
BF16 = jnp.bfloat16

STEPS = 32
STEPS_DEV = 8
HALF = 192
HIDDEN = 384
CHAN = 16
TOKENS = 256
TILES = 8
GROUP = 8
ITEMS = 118
GROUPS = TILES * ITEMS // GROUP
DEPTH = 128
PARTS = 2
PART = HIDDEN // PARTS
ORDER = (
    ('g', 0), ('q', 0), ('g', 1), ('p', 0), ('p', 1), ('p', 2), ('g', 2), ('p', 3), ('g', 3), ('q', 1),
    ('p', 4), ('g', 4), ('p', 5), ('g', 5), ('p', 6), ('q', 2), ('g', 6), ('p', 7), ('g', 7), ('p', 8),
    ('g', 8), ('q', 3), ('p', 9), ('g', 9), ('p', 10), ('g', 10), ('g', 11), ('p', 11), ('p', 12), ('g', 12),
    ('p', 13), ('g', 13), ('p', 14), ('g', 14), ('p', 15), ('g', 15),
)

ROOT = math.sqrt(2.0 / math.pi)
C1 = 2.0 * ROOT
C3 = 8.0 * 0.044715 * ROOT


def item(group, k):
    start = group * GROUP
    tile, n = lax.div(start, ITEMS), lax.rem(start, ITEMS) + k
    wrap = n >= ITEMS
    tile, n = jnp.where(wrap, tile + 1, tile), jnp.where(wrap, n - ITEMS, n)
    j = jnp.where(n < 31, n, jnp.where(n < 61, n - 30, jnp.where(n < 90, n - 59, n - 87)))
    return tile, n < 31, j


def kernel(x_ref, w1_ref, w2_ref, g_ref, b_ref, h_ref, out_ref,
           gam, bet, w1s, w2s, hs, hb, w1f, gamf, betf, mat, rhs, w2p, xs, pre_a, pre_b, act_a, act_b, lat,
           own_sem, psend, precv, send_sem, recv_sem):
    m = lax.axis_index("model")
    t = lax.axis_index("time")
    me = m * 4 + t

    offsets = [(dm, dt) for dm in range(2) for dt in range(4) if (dm, dt) != (0, 0)]
    peers = [(lax.rem(m + dm, 2), lax.rem(t + dt, 4)) for dm, dt in offsets]

    local = [pltpu.make_async_copy(src, dst, own_sem.at[i]) for i, (src, dst) in enumerate([
        (g_ref, gam.at[m, t]), (b_ref, bet.at[m, t]), (w1_ref, w1s.at[m]), (w2_ref, w2s.at[m]), (h_ref, hs.at[t]),
        (x_ref.at[pl.ds(me * TILES, TILES)], xs)])]
    for copy in local:
        copy.start()

    barrier = pltpu.get_barrier_semaphore()
    for pm, pt in peers:
        pl.semaphore_signal(barrier, inc=1, device_id={"model": pm, "time": pt}, device_id_type=MESH)
    pl.semaphore_wait(barrier, len(peers))

    copies = []

    def push(src, dst, peer):
        idx = len(copies)
        copy = pltpu.make_async_remote_copy(
            src_ref=src, dst_ref=dst, send_sem=psend.at[idx], recv_sem=precv.at[idx],
            device_id={"model": peer[0], "time": peer[1]}, device_id_type=MESH)
        copy.start()
        copies.append(copy)

    for (dm, dt), peer in zip(offsets, peers):
        push(g_ref, gam.at[m, t], peer)
        push(b_ref, bet.at[m, t], peer)
        if dt == 0:
            push(w1_ref, w1s.at[m], peer)
            push(w2_ref, w2s.at[m], peer)
        if dm == 0:
            push(h_ref, hs.at[t], peer)

    w1f[...] = jnp.zeros_like(w1f)
    w2p[...] = jnp.zeros_like(w2p)
    gamf[...] = jnp.zeros_like(gamf)
    betf[...] = jnp.zeros_like(betf)

    ones_zeros = jnp.concatenate([jnp.ones((16, TOKENS), BF16), jnp.zeros((DEPTH - 64, TOKENS), BF16)], axis=0)

    def init_slot(i, c):
        rhs[i, 48:DEPTH, :] = ones_zeros
        return c

    lax.fori_loop(0, STEPS + TILES, init_slot, 0)

    for copy in local:
        copy.wait()

    def init_tile(i, c):
        x0 = xs[i]
        lat[i, 0] = x0
        xb = x0.astype(BF16)
        for r in range(3):
            rhs[STEPS + i, 16 * r:16 * r + 16, :] = xb
        return c

    lax.fori_loop(0, TILES, init_tile, 0)

    for copy in copies:
        copy.wait()

    for mm in range(2):
        w1f[mm, :, 0:HALF] = w1s[mm].astype(F32) * 0.5
        for u in range(2):
            w2p[CHAN * u:CHAN * u + CHAN, 256 * u + 128 * mm:256 * u + 128 * mm + 128] = w2s[mm][:, 0:128]
        for tt in range(4):
            gamf[mm, 8 * tt:8 * tt + 8, 0:HALF] = gam[mm, tt].astype(F32)
            betf[mm, 8 * tt:8 * tt + 8, 0:HALF] = bet[mm, tt].astype(F32)

    for tt in range(4):
        for r in range(STEPS_DEV):
            hb[tt * STEPS_DEV + r] = jnp.broadcast_to(hs[tt, :, r:r + 1], (CHAN, TOKENS))

    tails = jnp.concatenate([w2s[mm].astype(F32)[:, 128:HALF] for mm in range(2)], axis=1).astype(BF16)
    for u in range(2):
        w2p[CHAN * u:CHAN * u + CHAN, 512 + 128 * u:640 + 128 * u] = tails

    row0 = lax.broadcasted_iota(jnp.int32, (8, 256), 0) == 0

    def prep(j, c):
        for mm in range(2):
            w = w1f[mm] * (1.0 + gamf[mm, pl.ds(j, 1), :])
            hi = w.astype(BF16).astype(F32)
            rest = w - hi
            mid = rest.astype(BF16).astype(F32)
            low = rest - mid
            shift = jnp.where(row0, 0.5 * betf[mm, pl.ds(j, 1), :], 0.0)
            cols = jnp.concatenate([hi, mid, low, shift, jnp.zeros((DEPTH - 56, 256), F32)], axis=0)
            mat[j, HALF * mm:HALF * mm + HALF, :] = cols.T[0:HALF, :].astype(BF16)
        return c

    lax.fori_loop(0, STEPS, prep, 0, unroll=4)

    def product1(group, pre, h):
        i, rows = h // PARTS, pl.ds(h % PARTS * PART, PART)
        tile, sweep0, j = item(group, i)
        slot = jnp.where(sweep0, STEPS + tile, j)
        pre[i, rows, :] = jnp.dot(mat[j, rows, :], rhs[slot], preferred_element_type=F32)

    def gelu(pre, act, h):
        i = h // PARTS
        u = i % 2
        for r in range(h % PARTS * PART, h % PARTS * PART + PART, 16):
            part, k = r // HALF, r % HALF
            row = u * 256 + part * 128 + k if k < 128 else 512 + u * 128 + part * 64 + k - 128
            z = pre[i, r:r + 16, :]
            f = z * (z * z * C3 + C1)
            act[i // 2, row:row + 16, :] = (z * (1.0 + jnp.tanh(f))).astype(BF16)

    def product2(act, pair):
        both = jnp.dot(w2p[...], act[pair], preferred_element_type=F32)
        return [both[0:CHAN], both[CHAN:2 * CHAN]]

    def update(group, spare, drifts):
        for i in range(GROUP):
            tile, _, j = item(group, i)
            tile = jnp.where(spare, TILES, tile)
            x = lat[tile, j] + hb[j] * drifts[i]
            lat[tile, j + 1] = x
            xb = x.astype(BF16)
            slot = jnp.where(spare, STEPS + TILES, j + 1)
            for r in range(3):
                rhs[slot, 16 * r:16 * r + 16, :] = xb

    pres, acts = [pre_a, pre_b], [act_a, act_b]

    def second_products(act):
        return [d for i in range(GROUP // 2) for d in product2(act, i)]

    def stage(index, parity):
        following = jnp.minimum(index + 1, GROUPS - 1)
        drifts = []
        for kind, i in ORDER:
            if kind == 'g':
                gelu(pres[parity], acts[parity], i)
            elif kind == 'p':
                product1(following, pres[1 - parity], i)
            else:
                drifts += product2(acts[1 - parity], i)
        update(jnp.maximum(index - 1, 0), index == 0, drifts)

    for h in range(PARTS * GROUP):
        product1(0, pre_a, h)

    def outgoing(tile, q, pm, slot):
        return pltpu.make_async_remote_copy(
            src_ref=lat.at[tile, pl.ds(q * STEPS_DEV, STEPS_DEV)],
            dst_ref=out_ref.at[:, me * TILES + tile],
            send_sem=send_sem.at[q, slot],
            recv_sem=recv_sem.at[me],
            device_id={"model": pm, "time": q}, device_id_type=MESH)

    def send(tile, q):
        outgoing(tile, q, 1 - m, 0).start()

        @pl.when(q != t)
        def _():
            outgoing(tile, q, m, 1).start()

        @pl.when(q == t)
        def _():
            for r in range(STEPS_DEV):
                out_ref[r, me * TILES + tile] = lat[tile, q * STEPS_DEV + r]

    def send_done(group):
        past = jnp.maximum(group * GROUP + GROUP - 1 - 93, 0)
        tile, rest = lax.div(past, ITEMS), lax.rem(past, ITEMS)

        @pl.when((group * GROUP + GROUP - 1 >= 93) & (rest < 32))
        def _():
            send(tile, lax.div(rest, 8))

    def trip(i, c):
        for parity in range(2):
            stage(2 * i + parity, parity)
            send_done(2 * i + parity - 1)
        return c

    lax.fori_loop(0, GROUPS // 2, trip, 0)
    update(GROUPS - 1, False, second_products(act_b))
    send(TILES - 1, 3)

    def waiter(q, slot, src):
        return pltpu.make_async_remote_copy(
            src_ref=lat.at[pl.ds(0, TILES), pl.ds(q * STEPS_DEV, STEPS_DEV)],
            dst_ref=out_ref.at[:, pl.ds(src * TILES, TILES)],
            send_sem=send_sem.at[q, slot],
            recv_sem=recv_sem.at[src],
            device_id={"model": 1 - m, "time": t}, device_id_type=MESH)

    for q in range(4):
        waiter(q, 0, 0).wait_send()

        @pl.when(q != t)
        def _():
            waiter(q, 1, 0).wait_send()

    for src in range(8):
        @pl.when(src != me)
        def _():
            waiter(0, 0, src).wait_recv()


def solution(mesh):
    def device_body(x_init, w_up, w_down, mod_scale, mod_shift, step_size):
        batch = x_init.shape[0]
        vmem = pl.BlockSpec(memory_space=pltpu.VMEM)
        hbm = pl.BlockSpec(memory_space=pltpu.HBM)
        out = pl.pallas_call(
            kernel,
            out_shape=pltpu.VMEM((STEPS_DEV, batch, CHAN, TOKENS), F32),
            in_specs=[hbm] * 6,
            out_specs=vmem,
            scratch_shapes=[
                pltpu.VMEM((2, 4, STEPS_DEV, HALF), BF16),
                pltpu.VMEM((2, 4, STEPS_DEV, HALF), BF16),
                pltpu.VMEM((2, CHAN, HALF), BF16),
                pltpu.VMEM((2, CHAN, HALF), BF16),
                pltpu.VMEM((4, 1, STEPS_DEV), F32),
                pltpu.VMEM((STEPS, CHAN, TOKENS), F32),
                pltpu.VMEM((2, CHAN, 256), F32),
                pltpu.VMEM((2, STEPS, 256), F32),
                pltpu.VMEM((2, STEPS, 256), F32),
                pltpu.VMEM((STEPS, HIDDEN, DEPTH), BF16),
                pltpu.VMEM((STEPS + TILES + 1, DEPTH, TOKENS), BF16),
                pltpu.VMEM((2 * CHAN, 2 * HIDDEN), BF16),
                pltpu.VMEM((TILES, CHAN, TOKENS), F32),
                pltpu.VMEM((GROUP, HIDDEN, TOKENS), F32),
                pltpu.VMEM((GROUP, HIDDEN, TOKENS), F32),
                pltpu.VMEM((GROUP // 2, 2 * HIDDEN, TOKENS), BF16),
                pltpu.VMEM((GROUP // 2, 2 * HIDDEN, TOKENS), BF16),
                pltpu.VMEM((TILES + 1, STEPS, CHAN, TOKENS), F32),
                pltpu.SemaphoreType.DMA((6,)),
                pltpu.SemaphoreType.DMA((19,)),
                pltpu.SemaphoreType.DMA((19,)),
                pltpu.SemaphoreType.DMA((4, 2)),
                pltpu.SemaphoreType.DMA((8,)),
            ],
            compiler_params=pltpu.CompilerParams(
                collective_id=0, has_side_effects=True, vmem_limit_bytes=32 * 1024 * 1024),
        )(*[pltpu.with_memory_space_constraint(a, pltpu.HBM) for a in (
            x_init.transpose(0, 2, 1), w_up, w_down.T, mod_scale, mod_shift, step_size[None, :])])
        return out.transpose(0, 1, 3, 2)

    return jax.shard_map(
        device_body, mesh=mesh,
        in_specs=(P('data', None, None), P(None, 'model'), P('model', None), P('time', 'model'), P('time', 'model'), P('time')),
        out_specs=P('time', 'data', None, None), check_vma=False)
```

```python
import functools
import math

import jax
import jax.numpy as jnp
from jax import lax
from jax.experimental import pallas as pl
from jax.experimental.pallas import tpu as pltpu
from jax.sharding import PartitionSpec as P

MESH = pl.DeviceIdType.MESH
F32 = jnp.float32
BF16 = jnp.bfloat16

STEPS = 32
STEPS_DEV = 8
HALF = 192
HIDDEN = 384
CHAN = 16
TOKENS = 256
TILES = 8
GROUP = 8
ITEMS = 118
GROUPS = TILES * ITEMS // GROUP
DEPTH = 128
PARTS = 2
PART = HIDDEN // PARTS
ORDER = (
    ('g', 0), ('q', 0), ('g', 1), ('p', 0), ('p', 1), ('p', 2), ('g', 2), ('p', 3), ('g', 3), ('q', 1),
    ('p', 4), ('g', 4), ('p', 5), ('g', 5), ('p', 6), ('q', 2), ('g', 6), ('p', 7), ('g', 7), ('p', 8),
    ('g', 8), ('q', 3), ('p', 9), ('g', 9), ('p', 10), ('g', 10), ('g', 11), ('p', 11), ('p', 12), ('g', 12),
    ('p', 13), ('g', 13), ('p', 14), ('g', 14), ('p', 15), ('g', 15),
)

ROOT = math.sqrt(2.0 / math.pi)
C1 = 2.0 * ROOT
C3 = 8.0 * 0.044715 * ROOT


def item(group, k):
    start = group * GROUP
    tile, n = lax.div(start, ITEMS), lax.rem(start, ITEMS) + k
    wrap = n >= ITEMS
    tile, n = jnp.where(wrap, tile + 1, tile), jnp.where(wrap, n - ITEMS, n)
    j = jnp.where(n < 31, n, jnp.where(n < 61, n - 30, jnp.where(n < 90, n - 59, n - 87)))
    return tile, n < 31, j


def kernel(x_ref, w1_ref, w2_ref, g_ref, b_ref, h_ref, out_ref,
           gam, bet, w1s, w2s, hs, hb, w1f, gamf, betf, mat, rhs, w2p, xs, pre_a, pre_b, act_a, act_b, lat,
           own_sem, psend, precv, send_sem, recv_sem):
    m = lax.axis_index("model")
    t = lax.axis_index("time")
    me = m * 4 + t

    offsets = [(dm, dt) for dm in range(2) for dt in range(4) if (dm, dt) != (0, 0)]
    peers = [(lax.rem(m + dm, 2), lax.rem(t + dt, 4)) for dm, dt in offsets]

    local = [pltpu.make_async_copy(src, dst, own_sem.at[i]) for i, (src, dst) in enumerate([
        (g_ref, gam.at[m, t]), (b_ref, bet.at[m, t]), (w1_ref, w1s.at[m]), (w2_ref, w2s.at[m]), (h_ref, hs.at[t]),
        (x_ref.at[pl.ds(me * TILES, TILES)], xs)])]
    for copy in local:
        copy.start()

    barrier = pltpu.get_barrier_semaphore()
    for pm, pt in peers:
        pl.semaphore_signal(barrier, inc=1, device_id={"model": pm, "time": pt}, device_id_type=MESH)
    pl.semaphore_wait(barrier, len(peers))

    copies = []

    def push(src, dst, peer):
        idx = len(copies)
        copy = pltpu.make_async_remote_copy(
            src_ref=src, dst_ref=dst, send_sem=psend.at[idx], recv_sem=precv.at[idx],
            device_id={"model": peer[0], "time": peer[1]}, device_id_type=MESH)
        copy.start()
        copies.append(copy)

    for (dm, dt), peer in zip(offsets, peers):
        push(g_ref, gam.at[m, t], peer)
        push(b_ref, bet.at[m, t], peer)
        if dt == 0:
            push(w1_ref, w1s.at[m], peer)
            push(w2_ref, w2s.at[m], peer)
        if dm == 0:
            push(h_ref, hs.at[t], peer)

    w1f[...] = jnp.zeros_like(w1f)
    w2p[...] = jnp.zeros_like(w2p)
    gamf[...] = jnp.zeros_like(gamf)
    betf[...] = jnp.zeros_like(betf)

    ones_zeros = jnp.concatenate([jnp.ones((16, TOKENS), BF16), jnp.zeros((DEPTH - 64, TOKENS), BF16)], axis=0)

    def init_slot(i, c):
        rhs[i, 48:DEPTH, :] = ones_zeros
        return c

    lax.fori_loop(0, STEPS + TILES, init_slot, 0)

    for copy in local:
        copy.wait()

    def init_tile(i, c):
        x0 = xs[i]
        lat[i, 0] = x0
        xb = x0.astype(BF16)
        for r in range(3):
            rhs[STEPS + i, 16 * r:16 * r + 16, :] = xb
        return c

    lax.fori_loop(0, TILES, init_tile, 0)

    for copy in copies:
        copy.wait()

    for mm in range(2):
        w1f[mm, :, 0:HALF] = w1s[mm].astype(F32) * 0.5
        for u in range(2):
            w2p[CHAN * u:CHAN * u + CHAN, 256 * u + 128 * mm:256 * u + 128 * mm + 128] = w2s[mm][:, 0:128]
        for tt in range(4):
            gamf[mm, 8 * tt:8 * tt + 8, 0:HALF] = gam[mm, tt].astype(F32)
            betf[mm, 8 * tt:8 * tt + 8, 0:HALF] = bet[mm, tt].astype(F32)

    for tt in range(4):
        for r in range(STEPS_DEV):
            hb[tt * STEPS_DEV + r] = jnp.broadcast_to(hs[tt, :, r:r + 1], (CHAN, TOKENS))

    tails = jnp.concatenate([w2s[mm].astype(F32)[:, 128:HALF] for mm in range(2)], axis=1).astype(BF16)
    for u in range(2):
        w2p[CHAN * u:CHAN * u + CHAN, 512 + 128 * u:640 + 128 * u] = tails

    row0 = lax.broadcasted_iota(jnp.int32, (8, 256), 0) == 0

    def prep(j, c):
        for mm in range(2):
            w = w1f[mm] * (1.0 + gamf[mm, pl.ds(j, 1), :])
            hi = w.astype(BF16).astype(F32)
            rest = w - hi
            mid = rest.astype(BF16).astype(F32)
            low = rest - mid
            shift = jnp.where(row0, 0.5 * betf[mm, pl.ds(j, 1), :], 0.0)
            cols = jnp.concatenate([hi, mid, low, shift, jnp.zeros((DEPTH - 56, 256), F32)], axis=0)
            mat[j, HALF * mm:HALF * mm + HALF, :] = cols.T[0:HALF, :].astype(BF16)
        return c

    lax.fori_loop(0, STEPS, prep, 0, unroll=8)

    def product1(group, pre, h):
        i, rows = h // PARTS, pl.ds(h % PARTS * PART, PART)
        tile, sweep0, j = item(group, i)
        slot = jnp.where(sweep0, STEPS + tile, j)
        pre[i, rows, :] = jnp.dot(mat[j, rows, :], rhs[slot], preferred_element_type=F32)

    def gelu(pre, act, h):
        i = h // PARTS
        u = i % 2
        for r in range(h % PARTS * PART, h % PARTS * PART + PART, 16):
            part, k = r // HALF, r % HALF
            row = u * 256 + part * 128 + k if k < 128 else 512 + u * 128 + part * 64 + k - 128
            z = pre[i, r:r + 16, :]
            f = z * (z * z * C3 + C1)
            act[i // 2, row:row + 16, :] = (z * (1.0 + jnp.tanh(f))).astype(BF16)

    def product2(act, pair):
        both = jnp.dot(w2p[...], act[pair], preferred_element_type=F32)
        return [both[0:CHAN], both[CHAN:2 * CHAN]]

    def update(group, spare, drifts):
        for i in range(GROUP):
            tile, _, j = item(group, i)
            tile = jnp.where(spare, TILES, tile)
            x = lat[tile, j] + hb[j] * drifts[i]
            lat[tile, j + 1] = x
            xb = x.astype(BF16)
            slot = jnp.where(spare, STEPS + TILES, j + 1)
            for r in range(3):
                rhs[slot, 16 * r:16 * r + 16, :] = xb

    pres, acts = [pre_a, pre_b], [act_a, act_b]

    def second_products(act):
        return [d for i in range(GROUP // 2) for d in product2(act, i)]

    def stage(index, parity):
        following = jnp.minimum(index + 1, GROUPS - 1)
        drifts = []
        for kind, i in ORDER:
            if kind == 'g':
                gelu(pres[parity], acts[parity], i)
            elif kind == 'p':
                product1(following, pres[1 - parity], i)
            else:
                drifts += product2(acts[1 - parity], i)
        update(jnp.maximum(index - 1, 0), index == 0, drifts)

    for h in range(PARTS * GROUP):
        product1(0, pre_a, h)

    def outgoing(tile, q, pm, slot):
        return pltpu.make_async_remote_copy(
            src_ref=lat.at[tile, pl.ds(q * STEPS_DEV, STEPS_DEV)],
            dst_ref=out_ref.at[:, me * TILES + tile],
            send_sem=send_sem.at[q, slot],
            recv_sem=recv_sem.at[me],
            device_id={"model": pm, "time": q}, device_id_type=MESH)

    def send(tile, q):
        outgoing(tile, q, 1 - m, 0).start()

        @pl.when(q != t)
        def _():
            outgoing(tile, q, m, 1).start()

        @pl.when(q == t)
        def _():
            for r in range(STEPS_DEV):
                out_ref[r, me * TILES + tile] = lat[tile, q * STEPS_DEV + r]

    def send_done(group):
        past = jnp.maximum(group * GROUP + GROUP - 1 - 93, 0)
        tile, rest = lax.div(past, ITEMS), lax.rem(past, ITEMS)

        @pl.when((group * GROUP + GROUP - 1 >= 93) & (rest < 32))
        def _():
            send(tile, lax.div(rest, 8))

    def trip(i, c):
        for parity in range(2):
            stage(2 * i + parity, parity)
            send_done(2 * i + parity - 1)
        return c

    lax.fori_loop(0, GROUPS // 2, trip, 0)
    update(GROUPS - 1, False, second_products(act_b))
    send(TILES - 1, 3)

    def waiter(q, slot, src):
        return pltpu.make_async_remote_copy(
            src_ref=lat.at[pl.ds(0, TILES), pl.ds(q * STEPS_DEV, STEPS_DEV)],
            dst_ref=out_ref.at[:, pl.ds(src * TILES, TILES)],
            send_sem=send_sem.at[q, slot],
            recv_sem=recv_sem.at[src],
            device_id={"model": 1 - m, "time": t}, device_id_type=MESH)

    for q in range(4):
        waiter(q, 0, 0).wait_send()

        @pl.when(q != t)
        def _():
            waiter(q, 1, 0).wait_send()

    for src in range(8):
        @pl.when(src != me)
        def _():
            waiter(0, 0, src).wait_recv()


def solution(mesh):
    def device_body(x_init, w_up, w_down, mod_scale, mod_shift, step_size):
        batch = x_init.shape[0]
        vmem = pl.BlockSpec(memory_space=pltpu.VMEM)
        hbm = pl.BlockSpec(memory_space=pltpu.HBM)
        out = pl.pallas_call(
            kernel,
            out_shape=pltpu.VMEM((STEPS_DEV, batch, CHAN, TOKENS), F32),
            in_specs=[hbm] * 6,
            out_specs=vmem,
            scratch_shapes=[
                pltpu.VMEM((2, 4, STEPS_DEV, HALF), BF16),
                pltpu.VMEM((2, 4, STEPS_DEV, HALF), BF16),
                pltpu.VMEM((2, CHAN, HALF), BF16),
                pltpu.VMEM((2, CHAN, HALF), BF16),
                pltpu.VMEM((4, 1, STEPS_DEV), F32),
                pltpu.VMEM((STEPS, CHAN, TOKENS), F32),
                pltpu.VMEM((2, CHAN, 256), F32),
                pltpu.VMEM((2, STEPS, 256), F32),
                pltpu.VMEM((2, STEPS, 256), F32),
                pltpu.VMEM((STEPS, HIDDEN, DEPTH), BF16),
                pltpu.VMEM((STEPS + TILES + 1, DEPTH, TOKENS), BF16),
                pltpu.VMEM((2 * CHAN, 2 * HIDDEN), BF16),
                pltpu.VMEM((TILES, CHAN, TOKENS), F32),
                pltpu.VMEM((GROUP, HIDDEN, TOKENS), F32),
                pltpu.VMEM((GROUP, HIDDEN, TOKENS), F32),
                pltpu.VMEM((GROUP // 2, 2 * HIDDEN, TOKENS), BF16),
                pltpu.VMEM((GROUP // 2, 2 * HIDDEN, TOKENS), BF16),
                pltpu.VMEM((TILES + 1, STEPS, CHAN, TOKENS), F32),
                pltpu.SemaphoreType.DMA((6,)),
                pltpu.SemaphoreType.DMA((19,)),
                pltpu.SemaphoreType.DMA((19,)),
                pltpu.SemaphoreType.DMA((4, 2)),
                pltpu.SemaphoreType.DMA((8,)),
            ],
            compiler_params=pltpu.CompilerParams(
                collective_id=0, has_side_effects=True, vmem_limit_bytes=32 * 1024 * 1024),
        )(*[pltpu.with_memory_space_constraint(a, pltpu.HBM) for a in (
            x_init.transpose(0, 2, 1), w_up, w_down.T, mod_scale, mod_shift, step_size[None, :])])
        return out.transpose(0, 1, 3, 2)

    return jax.shard_map(
        device_body, mesh=mesh,
        in_specs=(P('data', None, None), P(None, 'model'), P('model', None), P('time', 'model'), P('time', 'model'), P('time')),
        out_specs=P('time', 'data', None, None), check_vma=False)
```
